32 devices in a mesh: tok: 16 (over z, x, core), grp: 2 (over y).
Axes of the slice: x: 2, y: 2, z: 4, core: 2. Of those that a mesh axis runs over, the one named last changes fastest.
Arguments:
- queries: bfloat16 [2, 2048, 3072], P('grp', 'tok'), may hold values from -20 to 20, as said below
- keys: bfloat16 [2, 2048, 3072], P('grp', 'tok'), may hold values from -20 to 20, as said below
- values: bfloat16 [2, 2048, 3072], P('grp', 'tok'), may hold values from -10 to 10, as said below
- next_latent: bfloat16 [2, 2048, 3072], P('grp', 'tok'), may hold values from -20 to 20, as said below
- clip_blocks: int32 [2, 4], P('grp'), may hold values from 1 to 8, 16 in all within a row
- valid_counts: int32 [2, 16], P('grp'), may hold values from 32 to 128
- group_ids: int32 [2, 4], P('grp'), may hold values from 0 to 3
- rewards: float32 [2, 4], P('grp'), may hold values from -6 to 6
Outputs:
- velocity: bfloat16 [2, 2048, 3072], P('grp', 'tok')
- loss: float32 [], replicated
The draws below stay inside these ranges and needn't reach their ends.
Inputs may be any that keep to these rules, and one draw needn't show every extreme that they name: queries drawn within the range. keys drawn within the range. values drawn within the range. `next_latent`: next latents drawn within the range.
All inputs are finite; a program needn't handle non-finite values.
Results may differ from the reference program's by a relative error of at most 0.0034.
Values may be sent and summed in bfloat16 or wider, within the bound.
No kernel may reach another device: no remote copies, remote signals or barrier semaphores. Data moves between devices by JAX's collectives and lax.ppermute only.
A program may use at most 128 MiB of HBM per device.

```python
import math
import jax
import jax.numpy as jnp
import numpy as np
from jax import lax

D = 3072
HEADS = 24
HEAD = 128
BLK = 128
MAXB = 8
GROUPS = 4
NBT = 16
TOKENS = 2048
CLIPS = 4
N_GRP = 2


def paired_draw(key):
    shape = (N_GRP, TOKENS, D)
    key_part = jax.random.truncated_normal(jax.random.fold_in(key, 11), -6.0, 6.0, shape, jnp.float32)
    query_part = jax.random.truncated_normal(jax.random.fold_in(key, 12), -6.0, 6.0, shape, jnp.float32)
    return (query_part, key_part)


def draw_queries(key, part):
    return paired_draw(key)[0].astype(jnp.bfloat16)


def draw_keys(key, part):
    return paired_draw(key)[1].astype(jnp.bfloat16)


def draw_values(key, part):
    means_shape = (N_GRP, NBT, 1, D)
    noise_shape = (N_GRP, NBT, BLK, D)
    means = jax.random.truncated_normal(jax.random.fold_in(key, 32), -4.0, 4.0, means_shape, jnp.float32)
    noise = jax.random.truncated_normal(jax.random.fold_in(key, 33), -6.0, 6.0, noise_shape, jnp.float32)
    return (means + noise).reshape(N_GRP, TOKENS, D).astype(jnp.bfloat16)


def draw_next_latent(key, part):
    block_shape = (N_GRP, NBT, 1, 1)
    logs = jax.random.uniform(jax.random.fold_in(key, 21), block_shape, jnp.float32, jnp.log(0.3), jnp.log(3.0))
    noise = jax.random.truncated_normal(jax.random.fold_in(key, 22), -6.0, 6.0, (N_GRP, NBT, BLK, D), jnp.float32)
    latent = jnp.exp(logs) * noise
    return latent.reshape(N_GRP, TOKENS, D).astype(jnp.bfloat16)


def plant(result, stream_key, smallest, high):
    longest = result.shape.index(max(result.shape))
    spots = []
    for shift in (0, 1):
        where = [jax.random.randint(jax.random.fold_in(stream_key, axis), (), 0, length) for axis, length in enumerate(result.shape)]
        where[longest] = (where[longest] + shift) % result.shape[longest]
        spots.append(tuple(where))
    return result.at[spots[0]].set(smallest).at[spots[1]].set(high)


def block_levels(stream_key, shape, cuts, least, top_value):
    level, own = 1.0, jax.random.fold_in(stream_key, 6)
    for position, parts in cuts:
        steps = jnp.exp(jax.random.uniform(jax.random.fold_in(own, position), (parts,), jnp.float32, least / len(cuts), top_value / len(cuts)))
        level = level * jnp.repeat(steps, shape[position] // parts).reshape([-1 if axis == position else 1 for axis in range(len(shape))])
    return level


def profile(amount, total, most, slope):
    loads = [(1 << 20) // math.isqrt(standing ** slope) + 1 for standing in range(2, amount + 1)]
    spare, given = total - most - (amount - 1), [1] * (amount - 1)
    while spare > 0:
        candidates = [i for i in range(amount - 1) if given[i] < most]
        mass, budget = sum([loads[i] for i in candidates]), spare
        for i in candidates:
            more = min(most - given[i], max(1, budget * loads[i] // mass), spare)
            given[i] = given[i] + more
            spare = spare - more
    return np.array([most] + given)


def ragged(rng, count, total, limit, slope):
    if count == 2:
        one = jax.random.randint(rng, (), max(1, total - limit), min(limit, total - 1) + 1)
        return jnp.stack([one, total - one])
    tallies = jnp.asarray(profile(count, total, limit, slope), jnp.int32)
    twos = (count - 1) // 2
    giver, taker = tallies[1:1 + 2 * twos:2], tallies[2:2 + 2 * twos:2]
    slack = jnp.minimum(giver - 1, limit - taker)
    moved = jax.random.randint(jax.random.fold_in(rng, 1), (twos,), 0, 1 << 20) % (slack + 1)
    tallies = tallies.at[1:1 + 2 * twos:2].set(giver - moved).at[2:2 + 2 * twos:2].set(taker + moved)
    return tallies[jax.random.permutation(jax.random.fold_in(rng, 2), count)]


def gaussian(stream_key, shape, deviation, reach, pieces=(), held_as=jnp.bfloat16):
    array = jax.random.normal(stream_key, shape, jnp.float32) * deviation
    if len(pieces) > 0:
        array = block_levels(stream_key, shape, pieces, -0.22, 0.18) * array
    return jnp.clip(array, min=-reach, max=reach).astype(held_as)


def setup_inputs(seed: int = 0) -> dict:
    arg_keys = jax.random.split(jax.random.key(seed), 9)
    return {
        "queries": draw_queries(jax.random.fold_in(arg_keys[8], 71), 0),
        "keys": draw_keys(jax.random.fold_in(arg_keys[8], 71), 0),
        "values": draw_values(jax.random.fold_in(arg_keys[8], 71), 0),
        "next_latent": draw_next_latent(jax.random.fold_in(arg_keys[8], 71), 0),
        "clip_blocks": jax.vmap(lambda own: ragged(own, CLIPS, NBT, MAXB, 1))(jax.random.split(arg_keys[4], N_GRP)).reshape((N_GRP, CLIPS)).astype(jnp.int32),
        "valid_counts": plant(jax.random.randint(arg_keys[5], (N_GRP, NBT), BLK // 4, BLK + 1), jax.random.fold_in(arg_keys[5], 1), BLK // 4, BLK).astype(jnp.int32),
        "group_ids": plant(jax.random.randint(arg_keys[6], (N_GRP, CLIPS), 0, GROUPS), jax.random.fold_in(arg_keys[6], 1), 0, GROUPS - 1).astype(jnp.int32),
        "rewards": gaussian(arg_keys[7], (N_GRP, CLIPS), 1.0, 6.0, ((0, 2),), jnp.float32),
    }


masked_score = -1e+30

def block_clips(clip_row, total_blocks):
    ends = jnp.cumsum(clip_row).astype(jnp.int32)
    positions = jnp.arange(total_blocks, dtype=jnp.int32)
    return lax.optimization_barrier(jnp.sum((ends[None, :] <= positions[:, None]).astype(jnp.int32), axis=1)).astype(jnp.int32)

def advantages(reward_row, group_row):
    member = (group_row[:, None] == jnp.arange(GROUPS, dtype=jnp.int32)[None, :]).astype(jnp.float32)
    totals = lax.optimization_barrier(jnp.sum(member * reward_row[:, None], axis=0))
    counts = lax.optimization_barrier(jnp.sum(member, axis=0))
    means = totals / jnp.maximum(counts, 1.0)
    return reward_row - lax.optimization_barrier(jnp.sum(member * means[None, :], axis=1))

def clip_tokens(block_clip, valid_row, clips):
    member = (block_clip[:, None] == jnp.arange(clips, dtype=jnp.int32)[None, :]).astype(jnp.float32)
    return lax.optimization_barrier(jnp.sum(member * valid_row.astype(jnp.float32)[:, None], axis=0))

def attend(query_block, key_rows, value_rows, allowed):
    width = query_block.shape[0]
    count = key_rows.shape[0]
    query_heads = query_block.reshape(width, HEADS, HEAD).astype(jnp.float32)
    key_heads = key_rows.reshape(count, HEADS, HEAD).astype(jnp.float32)
    value_heads = value_rows.reshape(count, HEADS, HEAD).astype(jnp.float32)
    scores = jnp.einsum('qhd,khd->hqk', query_heads, key_heads) * (1.0 / math.sqrt(HEAD))
    scores = jnp.where(allowed[None, None, :], scores, masked_score)
    top = lax.optimization_barrier(jnp.max(scores, axis=-1, keepdims=True))
    expo = jnp.exp(scores - top)
    probs = (expo / lax.optimization_barrier(jnp.sum(expo, axis=-1, keepdims=True))).astype(jnp.bfloat16)
    mixed = jnp.einsum('hqk,khd->qhd', probs.astype(jnp.float32), value_heads)
    return mixed.reshape(width, HEADS * HEAD)

def row_velocity(query_row, key_row, value_row, clip_row, valid_row):
    total_blocks = valid_row.shape[0]
    block_clip = block_clips(clip_row, total_blocks)
    margin = (MAXB - 1) * BLK
    key_padded = jnp.pad(key_row, ((margin, margin), (0, 0)))
    value_padded = jnp.pad(value_row, ((margin, margin), (0, 0)))
    clip_padded = jnp.pad(block_clip, (MAXB - 1, MAXB - 1), constant_values=-1)
    valid_padded = jnp.pad(valid_row, (MAXB - 1, MAXB - 1))
    span = 2 * MAXB - 1

    def one_block(block):
        start = (block * BLK).astype(jnp.int32)
        query_block = lax.dynamic_slice_in_dim(query_row, start, BLK, 0)
        key_block = lax.dynamic_slice_in_dim(key_padded, start, span * BLK, 0)
        value_block = lax.dynamic_slice_in_dim(value_padded, start, span * BLK, 0)
        near_clips = lax.dynamic_slice_in_dim(clip_padded, block, span, 0)
        near_valid = lax.dynamic_slice_in_dim(valid_padded, block, span, 0)
        slots = jnp.arange(BLK, dtype=jnp.int32)
        allowed = (near_clips[:, None] == block_clip[block]) & (slots[None, :] < near_valid[:, None])
        mixed = attend(query_block, key_block, value_block, allowed.reshape(-1))
        live = slots < valid_row[block]
        return jnp.where(live[:, None], mixed, 0.0).astype(jnp.bfloat16)
    outputs = lax.map(one_block, jnp.arange(total_blocks, dtype=jnp.int32))
    return outputs.reshape(total_blocks * BLK, D)

def row_loss(velocity_row, next_row, clip_row, valid_row, group_row, reward_row):
    total_blocks = valid_row.shape[0]
    block_clip = block_clips(clip_row, total_blocks)
    diff = next_row.astype(jnp.float32) - velocity_row.astype(jnp.float32)
    token_err = lax.optimization_barrier(jnp.sum(diff * diff, axis=-1)).reshape(total_blocks, BLK)
    slots = jnp.arange(BLK, dtype=jnp.int32)
    live = (slots[None, :] < valid_row[:, None]).astype(jnp.float32)
    block_err = lax.optimization_barrier(jnp.sum(token_err * live, axis=1))
    adv = advantages(reward_row, group_row)
    tokens_of = clip_tokens(block_clip, valid_row, clip_row.shape[0])
    terms = jnp.take(adv, block_clip) * block_err / (2.0 * D * jnp.take(tokens_of, block_clip))
    return jnp.sum(terms)

def reference(queries, keys, values, next_latent, clip_blocks, valid_counts, group_ids, rewards):
    outputs = []
    total = jnp.zeros((), jnp.float32)
    for row in range(queries.shape[0]):
        velocity_row = row_velocity(queries[row], keys[row], values[row], clip_blocks[row], valid_counts[row])
        outputs.append(velocity_row)
        total = total + row_loss(velocity_row, next_latent[row], clip_blocks[row], valid_counts[row], group_ids[row], rewards[row])
    return (jnp.stack(outputs), total)
```

```python
import functools
import math

import jax
import jax.numpy as jnp
from jax import lax
from jax.experimental import pallas as pl
from jax.experimental.pallas import tpu as pltpu
from jax.sharding import PartitionSpec as P

HEADS = 24
HEAD = 128
BLK = 128
MAXB = 8
GROUPS = 4
LEVEL = MAXB // 2
REACH = MAXB - 1

masked_score = -1e30


def passed_along(value, axis, steps):
    count = lax.axis_size(axis)
    first, last = (max(0, -steps), min(count, count - steps))
    return lax.ppermute(value, axis, [(source, source + steps) for source in range(first, last)])


def advantages(reward_row, group_row):
    member = (group_row[:, None] == jnp.arange(GROUPS, dtype=jnp.int32)[None, :]).astype(
        jnp.float32
    )
    totals = jnp.sum(member * reward_row[:, None], axis=0)
    counts = jnp.sum(member, axis=0)
    means = totals / jnp.maximum(counts, 1.0)
    return reward_row - jnp.sum(member * means[None, :], axis=1)


def kernel_body(pieces, heads, start_ref, live_ref, weight_ref, bias_ref, *refs):
    parts = len(pieces)
    q_hbm, n_hbm = refs[0], refs[1]
    k_parts, v_parts = refs[2 : 2 + parts], refs[2 + parts : 2 + 2 * parts]
    out_ref, err_ref = refs[2 + 2 * parts], refs[3 + 2 * parts]
    q_buf, n_buf, k_buf, v_buf, sems = refs[4 + 2 * parts :]
    copies = [
        pltpu.make_async_copy(q_hbm, q_buf, sems.at[0]),
        pltpu.make_async_copy(n_hbm, n_buf, sems.at[1]),
    ]
    for index, (first, count) in enumerate(pieces):
        rows = pl.ds(first * BLK, count * BLK)
        copies.append(
            pltpu.make_async_copy(k_parts[index], k_buf.at[rows], sems.at[2 + 2 * index])
        )
        copies.append(
            pltpu.make_async_copy(v_parts[index], v_buf.at[rows], sems.at[3 + 2 * index])
        )
    for copy in copies:
        copy.start()
    for copy in copies:
        copy.wait()
    factor = math.log2(math.e) / math.sqrt(HEAD)
    err_ref[...] = jnp.zeros_like(err_ref)

    def one_block(block, carry):
        rows = pl.ds(pl.multiple_of(block * BLK, BLK), BLK)
        window = pl.ds(pl.multiple_of(start_ref[block] * BLK, BLK), MAXB * BLK)
        bias = bias_ref[pl.ds(block, 1), :]
        live = lax.broadcasted_iota(jnp.int32, (BLK, HEAD), 0) < live_ref[block]
        block_err = jnp.zeros((BLK, HEAD), jnp.float32)
        for head in range(heads):
            columns = slice(head * HEAD, (head + 1) * HEAD)
            scores = lax.dot_general(
                q_buf[rows, columns],
                k_buf[window, columns],
                (((1,), (1,)), ((), ())),
                preferred_element_type=jnp.float32,
            )
            scores = scores + bias
            top = jnp.max(scores, axis=-1, keepdims=True)
            expo = jnp.exp2((scores - top) * factor)
            probs = (expo * (1.0 / jnp.sum(expo, axis=-1, keepdims=True))).astype(jnp.bfloat16)
            mixed = lax.dot_general(
                probs,
                v_buf[window, columns],
                (((1,), (0,)), ((), ())),
                preferred_element_type=jnp.float32,
            )
            result = jnp.where(live, mixed, 0.0).astype(jnp.bfloat16)
            out_ref[rows, columns] = result
            diff = n_buf[rows, columns].astype(jnp.float32) - result.astype(jnp.float32)
            block_err = block_err + diff * diff
        block_err = jnp.where(live, block_err, 0.0)
        err_ref[...] += weight_ref[block] * jnp.sum(
            block_err.reshape(BLK // 8, 8, HEAD), axis=0
        )
        return carry

    lax.fori_loop(0, LEVEL, one_block, 0)


def attend(pieces, start, live, weight, bias, q, n, k_parts, v_parts):
    total = sum(count for _, count in pieces)
    width = q.shape[1]
    smem = pl.BlockSpec(memory_space=pltpu.SMEM)
    vmem = pl.BlockSpec(memory_space=pltpu.VMEM)
    hbm = pl.BlockSpec(memory_space=pl.ANY)
    parts = len(pieces)
    return pl.pallas_call(
        functools.partial(kernel_body, pieces, width // HEAD),
        out_shape=(
            jax.ShapeDtypeStruct(q.shape, jnp.bfloat16),
            jax.ShapeDtypeStruct((8, HEAD), jnp.float32),
        ),
        in_specs=[smem, smem, smem, vmem] + [hbm] * (2 + 2 * parts),
        out_specs=(vmem, vmem),
        scratch_shapes=[
            pltpu.VMEM(q.shape, jnp.bfloat16),
            pltpu.VMEM(q.shape, jnp.bfloat16),
            pltpu.VMEM((total * BLK, width), jnp.bfloat16),
            pltpu.VMEM((total * BLK, width), jnp.bfloat16),
            pltpu.SemaphoreType.DMA((2 + 2 * parts,)),
        ],
        compiler_params=pltpu.CompilerParams(vmem_limit_bytes=48 * 1024 * 1024),
        name="window_attention",
    )(start, live, weight, bias, q, n, *k_parts, *v_parts)


def on_device(queries, keys, values, next_latent, clip_blocks, valid_counts, group_ids, rewards):
    devices = lax.axis_size("tok")
    own_index = lax.axis_index("tok")
    width = queries.shape[2]
    levels = [list(range(first, first + LEVEL)) for first in range(0, devices, LEVEL)]

    def exchange(value):
        return lax.all_to_all(value, "tok", 1, 0, axis_index_groups=levels, tiled=True)

    valid_row = valid_counts[0]
    clip_row = clip_blocks[0]
    total_blocks = valid_row.shape[0]
    ends = jnp.cumsum(clip_row)
    starts = ends - clip_row
    positions = jnp.arange(total_blocks, dtype=jnp.int32)
    member = (starts[None, :] <= positions[:, None]) & (positions[:, None] < ends[None, :])
    tokens_of = jnp.sum(jnp.where(member, valid_row[:, None], 0), axis=0).astype(jnp.float32)
    clip_weight = advantages(rewards[0], group_ids[0]) / (2.0 * width * tokens_of)
    level_first = own_index // LEVEL * LEVEL
    own_ids = level_first + jnp.arange(LEVEL, dtype=jnp.int32)
    own_member = (starts[None, :] <= own_ids[:, None]) & (own_ids[:, None] < ends[None, :])
    own_start = jnp.sum(jnp.where(own_member, starts[None, :], 0), axis=1)
    own_count = jnp.sum(jnp.where(own_member, clip_row[None, :], 0), axis=1)
    own_weight = jnp.sum(jnp.where(own_member, clip_weight[None, :], 0.0), axis=1)
    own_live = jnp.take(valid_row, own_ids)
    near_ids = own_start[:, None] + jnp.arange(MAXB, dtype=jnp.int32)[None, :]
    near_live = jnp.take(valid_row, jnp.minimum(near_ids, total_blocks - 1))
    near_live = jnp.where(jnp.arange(MAXB)[None, :] < own_count[:, None], near_live, 0)
    slots = jnp.arange(BLK, dtype=jnp.int32)
    bias = jnp.where(slots[None, None, :] < near_live[:, :, None], 0.0, masked_score)
    bias = bias.astype(jnp.float32).reshape(LEVEL, MAXB * BLK)
    start = own_start - (level_first - REACH)

    def gathered(value):
        own = exchange(value[0])
        found = [(REACH, LEVEL, own)]
        upward = downward = own
        held = LEVEL
        for distance in range(1, -(-REACH // LEVEL) + 1):
            count = min(LEVEL, REACH - (distance - 1) * LEVEL)
            upward = passed_along(upward[(held - count) * BLK :], "tok", LEVEL)
            downward = passed_along(downward[: count * BLK], "tok", -LEVEL)
            held = count
            up_first = max(0, REACH - distance * LEVEL)
            found.append((up_first, count, upward))
            found.append((REACH + distance * LEVEL, count, downward))
        return found

    key_found = gathered(keys)
    value_found = gathered(values)
    q = exchange(queries[0])
    n = exchange(next_latent[0])
    pieces = tuple((first, count) for first, count, _ in key_found)
    out, err = attend(
        pieces,
        start,
        own_live,
        own_weight,
        bias,
        q,
        n,
        [piece for _, _, piece in key_found],
        [piece for _, _, piece in value_found],
    )
    velocity = lax.all_to_all(out, "tok", 0, 1, axis_index_groups=levels, tiled=True)
    share = jnp.sum(err)
    everyone = devices * lax.axis_size("grp")
    spread = jnp.full((everyone, HEAD), share)
    total = jnp.sum(lax.all_to_all(spread, ("tok", "grp"), 0, 0, tiled=True)[:, 0])
    return (velocity[None], total)


def solution(mesh):
    return jax.shard_map(
        on_device,
        mesh=mesh,
        in_specs=(
            P("grp", "tok", None),
            P("grp", "tok", None),
            P("grp", "tok", None),
            P("grp", "tok", None),
            P("grp", None),
            P("grp", None),
            P("grp", None),
            P("grp", None),
        ),
        out_specs=(P("grp", "tok", None), P()),
        check_vma=False,
    )
```

```python
import functools
import math

import jax
import jax.numpy as jnp
from jax import lax
from jax.experimental import pallas as pl
from jax.experimental.pallas import tpu as pltpu
from jax.sharding import PartitionSpec as P


HEAD = 128
BLK = 128
MAXB = 8
GROUPS = 4
LEVEL = MAXB // 2
REACH = MAXB - 1
CHUNKS = (1, 1)

masked_score = -1e30


def passed_along(value, axis, steps):
    count = lax.axis_size(axis)
    first, last = (max(0, -steps), min(count, count - steps))
    return lax.ppermute(value, axis, [(source, source + steps) for source in range(first, last)])


def advantages(reward_row, group_row):
    member = (group_row[:, None] == jnp.arange(GROUPS, dtype=jnp.int32)[None, :]).astype(
        jnp.float32
    )
    totals = jnp.sum(member * reward_row[:, None], axis=0)
    counts = jnp.sum(member, axis=0)
    means = totals / jnp.maximum(counts, 1.0)
    return reward_row - jnp.sum(member * means[None, :], axis=1)


def moved(copies):
    for copy in copies:
        copy.start()
    for copy in copies:
        copy.wait()


def pack_body(spans, first_ref, second_ref, *refs):
    outs, sems = refs[:-1], refs[-1]
    share = first_ref.shape[2] // LEVEL
    copies = []
    for out_ref, (low, high) in zip(outs, spans):
        for part in range(LEVEL):
            for side, ref in enumerate((first_ref, second_ref)):
                copies.append(
                    pltpu.make_async_copy(
                        ref.at[0, :, pl.ds(part * share + low, high - low)],
                        out_ref.at[part, :, pl.ds(side * (high - low), high - low)],
                        sems.at[len(copies)],
                    )
                )
    moved(copies)


def packed(first, second, spans):
    rows = first.shape[1]
    hbm = pl.BlockSpec(memory_space=pl.ANY)
    return pl.pallas_call(
        functools.partial(pack_body, spans),
        out_shape=[
            jax.ShapeDtypeStruct((LEVEL, rows, 2 * (high - low)), first.dtype)
            for low, high in spans
        ],
        in_specs=[hbm, hbm],
        out_specs=[hbm] * len(spans),
        scratch_shapes=[pltpu.SemaphoreType.DMA((2 * LEVEL * len(spans),))],
    )(first, second)


def unpack_body(spans, place_ref, *refs):
    parts, out_ref, sems = refs[:-2], refs[-2], refs[-1]
    share = out_ref.shape[2] // LEVEL
    own = place_ref[1]
    copies = []
    for index, (low, high) in enumerate(spans):
        for step in range(LEVEL):
            first = pl.multiple_of(jnp.bitwise_xor(own, step) * share + low, HEAD)
            copies.append(
                pltpu.make_async_copy(
                    parts[index * LEVEL + step],
                    out_ref.at[0, :, pl.ds(first, high - low)],
                    sems.at[len(copies)],
                )
            )
    moved(copies)


def unpacked(place, outs, spans, width):
    hbm = pl.BlockSpec(memory_space=pl.ANY)
    return pl.pallas_call(
        functools.partial(unpack_body, spans),
        out_shape=jax.ShapeDtypeStruct((1, outs[0].shape[0], width), outs[0].dtype),
        in_specs=[pl.BlockSpec(memory_space=pltpu.SMEM)] + [hbm] * len(outs),
        out_specs=hbm,
        scratch_shapes=[pltpu.SemaphoreType.DMA((len(outs),))],
        name="unpack",
    )(place, *outs)


def kernel_body(
    pieces, heads, first_head, place_ref, clip_ref, valid_ref, weight_ref, *refs
):
    parts = len(pieces)
    width = heads * HEAD
    qn_hbm = refs[0]
    kv_parts = refs[1 : 1 + parts]
    out_refs = refs[1 + parts : 1 + parts + LEVEL]
    err_ref, q_buf, n_buf, kv_buf, sems = refs[1 + parts + LEVEL :]
    half = qn_hbm.shape[1] // 2
    copies = [
        pltpu.make_async_copy(
            qn_hbm.at[:, pl.ds(first_head * HEAD, width)], q_buf, sems.at[0]
        ),
        pltpu.make_async_copy(
            qn_hbm.at[:, pl.ds(half + first_head * HEAD, width)], n_buf, sems.at[1]
        ),
    ]
    for index, (first, count) in enumerate(pieces):
        rows = pl.ds(first * BLK, count * BLK)
        copies.append(
            pltpu.make_async_copy(kv_parts[index], kv_buf.at[rows], sems.at[2 + index])
        )
    moved(copies)
    factor = math.log2(math.e) / math.sqrt(HEAD)
    err_ref[...] = jnp.zeros_like(err_ref)
    level_first, own = place_ref[0], place_ref[1]
    last_block = valid_ref.shape[1] - 1
    slots = lax.broadcasted_iota(jnp.int32, (1, BLK), 1)

    for step in range(LEVEL):
        block = jnp.bitwise_xor(own, step)
        own_id = level_first + block
        clip_start = clip_count = clip_first = jnp.int32(0)
        for clip in range(clip_ref.shape[1]):
            blocks = clip_ref[0, clip]
            mine = (own_id >= clip_first) & (own_id < clip_first + blocks)
            clip_start = jnp.where(mine, clip_first, clip_start)
            clip_count = jnp.where(mine, blocks, clip_count)
            clip_first = clip_first + blocks
        bias = []
        for near in range(MAXB):
            live = valid_ref[0, jnp.minimum(clip_start + near, last_block)]
            live = jnp.where(near < clip_count, live, 0)
            bias.append(jnp.where(slots < live, 0.0, masked_score).astype(jnp.float32))
        bias = jnp.concatenate(bias, axis=1)
        rows = pl.ds(pl.multiple_of(block * BLK, BLK), BLK)
        window_first = clip_start - (level_first - REACH)
        window = pl.ds(pl.multiple_of(window_first * BLK, BLK), MAXB * BLK)
        own_live = lax.broadcasted_iota(jnp.int32, (BLK, HEAD), 0) < valid_ref[0, own_id]
        block_err = jnp.zeros((BLK, HEAD), jnp.float32)
        for head in range(heads):
            columns = slice(head * HEAD, (head + 1) * HEAD)
            scores = lax.dot_general(
                q_buf[rows, columns],
                kv_buf[window, columns],
                (((1,), (1,)), ((), ())),
                preferred_element_type=jnp.float32,
            )
            scores = scores + bias
            top = jnp.max(scores, axis=-1, keepdims=True)
            expo = jnp.exp2((scores - top) * factor)
            probs = (expo * (1.0 / jnp.sum(expo, axis=-1, keepdims=True))).astype(jnp.bfloat16)
            mixed = lax.dot_general(
                probs,
                kv_buf[window, width + head * HEAD : width + (head + 1) * HEAD],
                (((1,), (0,)), ((), ())),
                preferred_element_type=jnp.float32,
            )
            result = jnp.where(own_live, mixed, 0.0).astype(jnp.bfloat16)
            out_refs[step][:, columns] = result
            diff = n_buf[rows, columns].astype(jnp.float32) - result.astype(jnp.float32)
            block_err = block_err + diff * diff
        block_err = jnp.where(own_live, block_err, 0.0)
        err_ref[...] += weight_ref[block] * jnp.sum(
            block_err.reshape(BLK // 8, 8, HEAD), axis=0
        )


def attend(pieces, first_head, tables, qn, kv_parts):
    total = sum(count for _, count in pieces)
    width = kv_parts[0].shape[1] // 2
    block_rows = qn.shape[0]
    smem = pl.BlockSpec(memory_space=pltpu.SMEM)
    vmem = pl.BlockSpec(memory_space=pltpu.VMEM)
    hbm = pl.BlockSpec(memory_space=pl.ANY)
    parts = len(pieces)
    units = LEVEL * (width // HEAD)
    return pl.pallas_call(
        functools.partial(kernel_body, pieces, width // HEAD, first_head),
        out_shape=[jax.ShapeDtypeStruct((BLK, width), jnp.bfloat16)] * LEVEL
        + [jax.ShapeDtypeStruct((8, HEAD), jnp.float32)],
        in_specs=[smem] * len(tables) + [hbm] * (1 + parts),
        out_specs=[vmem] * (LEVEL + 1),
        scratch_shapes=[
            pltpu.VMEM((block_rows, width), jnp.bfloat16),
            pltpu.VMEM((block_rows, width), jnp.bfloat16),
            pltpu.VMEM((total * BLK, 2 * width), jnp.bfloat16),
            pltpu.SemaphoreType.DMA((2 + parts,)),
        ],
        cost_estimate=pl.CostEstimate(
            flops=units * 4 * BLK * MAXB * BLK * HEAD,
            transcendentals=units * BLK * MAXB * BLK,
            bytes_accessed=4 * (total * BLK + 2 * block_rows) * width,
        ),
        compiler_params=pltpu.CompilerParams(vmem_limit_bytes=32 * 1024 * 1024),
    )(*tables, qn, *kv_parts)


def step(queries, keys, values, next_latent, clip_blocks, valid_counts, group_ids, rewards):
    devices = lax.axis_size("tok")
    own_index = lax.axis_index("tok")
    _, width = queries.shape[1:]
    share = width // LEVEL
    levels = [list(range(first, first + LEVEL)) for first in range(0, devices, LEVEL)]
    heads = share // HEAD
    cuts = [0]
    for part in CHUNKS:
        cuts.append(cuts[-1] + heads * part // sum(CHUNKS))
    spans = [(low * HEAD, high * HEAD) for low, high in zip(cuts[:-1], cuts[1:])]

    def exchange(value):
        return lax.all_to_all(value, "tok", 0, 0, axis_index_groups=levels, tiled=True)

    def exchanged(value):
        found = exchange(value)
        return found.reshape(found.shape[0] * found.shape[1], found.shape[2])

    def gathered(own):
        found = [(REACH, LEVEL, own)]
        upward = downward = own
        held = LEVEL
        for distance in range(1, -(-REACH // LEVEL) + 1):
            count = min(LEVEL, REACH - (distance - 1) * LEVEL)
            upward = passed_along(upward[(held - count) * BLK :], "tok", LEVEL)
            downward = passed_along(downward[: count * BLK], "tok", -LEVEL)
            held = count
            found.append((max(0, REACH - distance * LEVEL), count, upward))
            found.append((REACH + distance * LEVEL, count, downward))
        return found

    own_kv = []
    for span in spans:
        parts = packed(keys, values, [span])
        own_kv += [exchanged(part) for part in parts]
    (part,) = packed(queries, next_latent, [(0, share)])
    qn = exchanged(part)

    valid_row = valid_counts[0]
    clip_row = clip_blocks[0]
    ends = jnp.cumsum(clip_row)
    starts = ends - clip_row
    positions = jnp.arange(valid_row.shape[0], dtype=jnp.int32)
    member = (starts[None, :] <= positions[:, None]) & (positions[:, None] < ends[None, :])
    tokens_of = jnp.sum(jnp.where(member, valid_row[:, None], 0), axis=0).astype(jnp.float32)
    clip_weight = advantages(rewards[0], group_ids[0]) / (2.0 * width * tokens_of)
    level_first = own_index // LEVEL * LEVEL
    own_ids = level_first + jnp.arange(LEVEL, dtype=jnp.int32)
    own_member = (starts[None, :] <= own_ids[:, None]) & (own_ids[:, None] < ends[None, :])
    own_weight = jnp.sum(jnp.where(own_member, clip_weight[None, :], 0.0), axis=1)
    place = jnp.stack([level_first, own_index - level_first])
    tables = (place, clip_blocks, valid_counts, own_weight)

    outs, errs = [], []
    for (low, high), own in zip(spans, own_kv):
        found = gathered(own)
        pieces = tuple((first, count) for first, count, _ in found)
        *out, err = attend(pieces, low // HEAD, tables, qn, [piece for _, _, piece in found])
        outs.append(out[0])
        for step in range(1, LEVEL):
            partners = [(source, source ^ step) for source in range(devices)]
            outs.append(lax.ppermute(out[step], "tok", partners))
        errs.append(err)
    velocity = unpacked(place, outs, spans, width)
    device_share = jnp.sum(sum(errs))
    everyone = devices * lax.axis_size("grp")
    spread = jnp.full((everyone, HEAD), device_share)
    total = jnp.sum(lax.all_to_all(spread, ("tok", "grp"), 0, 0, tiled=True)[:, 0])
    return (velocity, total)


def solution(mesh):
    return jax.shard_map(
        step,
        mesh=mesh,
        in_specs=(
            P("grp", "tok", None),
            P("grp", "tok", None),
            P("grp", "tok", None),
            P("grp", "tok", None),
            P("grp", None),
            P("grp", None),
            P("grp", None),
            P("grp", None),
        ),
        out_specs=(P("grp", "tok", None), P()),
        check_vma=False,
    )
```

```python
import functools
import math

import jax
import jax.numpy as jnp
from jax import lax
from jax.experimental import pallas as pl
from jax.experimental.pallas import tpu as pltpu
from jax.sharding import PartitionSpec as P


HEAD = 128
BLK = 128
MAXB = 8
GROUPS = 4
LEVEL = MAXB // 2
REACH = MAXB - 1
CHUNKS = (1, 1)

masked_score = -1e30


def passed_along(value, axis, steps):
    count = lax.axis_size(axis)
    first, last = (max(0, -steps), min(count, count - steps))
    return lax.ppermute(value, axis, [(source, source + steps) for source in range(first, last)])


def advantages(reward_row, group_row):
    member = (group_row[:, None] == jnp.arange(GROUPS, dtype=jnp.int32)[None, :]).astype(
        jnp.float32
    )
    totals = jnp.sum(member * reward_row[:, None], axis=0)
    counts = jnp.sum(member, axis=0)
    means = totals / jnp.maximum(counts, 1.0)
    return reward_row - jnp.sum(member * means[None, :], axis=1)


def moved(copies):
    for copy in copies:
        copy.start()
    for copy in copies:
        copy.wait()


def pack_body(low, high, first_ref, second_ref, out_ref):
    share = first_ref.shape[2] // LEVEL
    span = high - low
    for part in range(LEVEL):
        for side, ref in enumerate((first_ref, second_ref)):
            out_ref[part, :, side * span : (side + 1) * span] = ref[
                0, :, part * share + low : part * share + high
            ]


def packed(first, second, low, high):
    vmem = pl.BlockSpec(memory_space=pltpu.VMEM)
    return pl.pallas_call(
        functools.partial(pack_body, low, high),
        out_shape=jax.ShapeDtypeStruct((LEVEL, first.shape[1], 2 * (high - low)), first.dtype),
        in_specs=[vmem, vmem],
        out_specs=vmem,
    )(first, second)


def unpack_body(spans, place_ref, *refs):
    parts, out_ref = refs[:-1], refs[-1]
    share = out_ref.shape[2] // LEVEL
    for index, (low, high) in enumerate(spans):
        for step in range(LEVEL):
            first = pl.multiple_of(jnp.bitwise_xor(place_ref[1], step) * share + low, HEAD)
            out_ref[0, :, pl.ds(first, high - low)] = parts[index * LEVEL + step][...]


def unpacked(place, outs, spans, width):
    vmem = pl.BlockSpec(memory_space=pltpu.VMEM)
    return pl.pallas_call(
        functools.partial(unpack_body, spans),
        out_shape=jax.ShapeDtypeStruct((1, outs[0].shape[0], width), outs[0].dtype),
        in_specs=[pl.BlockSpec(memory_space=pltpu.SMEM)] + [vmem] * len(outs),
        out_specs=vmem,
        name="unpack",
    )(place, *outs)


def kernel_body(
    pieces, heads, first_head, place_ref, clip_ref, valid_ref, weight_ref, *refs
):
    parts = len(pieces)
    width = heads * HEAD
    qn_hbm = refs[0]
    kv_parts = refs[1 : 1 + parts]
    out_refs = refs[1 + parts : 1 + parts + LEVEL]
    err_ref, q_buf, n_buf, kv_buf, sems = refs[1 + parts + LEVEL :]
    half = qn_hbm.shape[1] // 2
    copies = [
        pltpu.make_async_copy(
            qn_hbm.at[:, pl.ds(first_head * HEAD, width)], q_buf, sems.at[0]
        ),
        pltpu.make_async_copy(
            qn_hbm.at[:, pl.ds(half + first_head * HEAD, width)], n_buf, sems.at[1]
        ),
    ]
    for index, (first, count) in enumerate(pieces):
        rows = pl.ds(first * BLK, count * BLK)
        copies.append(
            pltpu.make_async_copy(kv_parts[index], kv_buf.at[rows], sems.at[2 + index])
        )
    moved(copies)
    factor = math.log2(math.e) / math.sqrt(HEAD)
    err_ref[...] = jnp.zeros_like(err_ref)
    level_first, own = place_ref[0], place_ref[1]
    last_block = valid_ref.shape[1] - 1
    slots = lax.broadcasted_iota(jnp.int32, (1, BLK), 1)

    for step in range(LEVEL):
        block = jnp.bitwise_xor(own, step)
        own_id = level_first + block
        clip_start = clip_count = clip_first = jnp.int32(0)
        for clip in range(clip_ref.shape[1]):
            blocks = clip_ref[0, clip]
            mine = (own_id >= clip_first) & (own_id < clip_first + blocks)
            clip_start = jnp.where(mine, clip_first, clip_start)
            clip_count = jnp.where(mine, blocks, clip_count)
            clip_first = clip_first + blocks
        bias = []
        for near in range(MAXB):
            live = valid_ref[0, jnp.minimum(clip_start + near, last_block)]
            live = jnp.where(near < clip_count, live, 0)
            bias.append(jnp.where(slots < live, 0.0, masked_score).astype(jnp.float32))
        bias = jnp.concatenate(bias, axis=1)
        rows = pl.ds(pl.multiple_of(block * BLK, BLK), BLK)
        window_first = clip_start - (level_first - REACH)
        window = pl.ds(pl.multiple_of(window_first * BLK, BLK), MAXB * BLK)
        own_live = lax.broadcasted_iota(jnp.int32, (BLK, HEAD), 0) < valid_ref[0, own_id]
        block_err = jnp.zeros((BLK, HEAD), jnp.float32)
        for head in range(heads):
            columns = slice(head * HEAD, (head + 1) * HEAD)
            scores = lax.dot_general(
                q_buf[rows, columns],
                kv_buf[window, columns],
                (((1,), (1,)), ((), ())),
                preferred_element_type=jnp.float32,
            )
            scores = scores + bias
            top = jnp.max(scores, axis=-1, keepdims=True)
            expo = jnp.exp2((scores - top) * factor)
            probs = (expo * (1.0 / jnp.sum(expo, axis=-1, keepdims=True))).astype(jnp.bfloat16)
            mixed = lax.dot_general(
                probs,
                kv_buf[window, width + head * HEAD : width + (head + 1) * HEAD],
                (((1,), (0,)), ((), ())),
                preferred_element_type=jnp.float32,
            )
            result = jnp.where(own_live, mixed, 0.0).astype(jnp.bfloat16)
            out_refs[step][:, columns] = result
            diff = n_buf[rows, columns].astype(jnp.float32) - result.astype(jnp.float32)
            block_err = block_err + diff * diff
        block_err = jnp.where(own_live, block_err, 0.0)
        err_ref[...] += weight_ref[block] * jnp.sum(
            block_err.reshape(BLK // 8, 8, HEAD), axis=0
        )


def attend(pieces, first_head, tables, qn, kv_parts):
    total = sum(count for _, count in pieces)
    width = kv_parts[0].shape[1] // 2
    block_rows = qn.shape[0]
    smem = pl.BlockSpec(memory_space=pltpu.SMEM)
    vmem = pl.BlockSpec(memory_space=pltpu.VMEM)
    hbm = pl.BlockSpec(memory_space=pl.ANY)
    parts = len(pieces)
    units = LEVEL * (width // HEAD)
    return pl.pallas_call(
        functools.partial(kernel_body, pieces, width // HEAD, first_head),
        out_shape=[jax.ShapeDtypeStruct((BLK, width), jnp.bfloat16)] * LEVEL
        + [jax.ShapeDtypeStruct((8, HEAD), jnp.float32)],
        in_specs=[smem] * len(tables) + [hbm] * (1 + parts),
        out_specs=[vmem] * (LEVEL + 1),
        scratch_shapes=[
            pltpu.VMEM((block_rows, width), jnp.bfloat16),
            pltpu.VMEM((block_rows, width), jnp.bfloat16),
            pltpu.VMEM((total * BLK, 2 * width), jnp.bfloat16),
            pltpu.SemaphoreType.DMA((2 + parts,)),
        ],
        cost_estimate=pl.CostEstimate(
            flops=units * 4 * BLK * MAXB * BLK * HEAD,
            transcendentals=units * BLK * MAXB * BLK,
            bytes_accessed=4 * (total * BLK + 2 * block_rows) * width,
        ),
        compiler_params=pltpu.CompilerParams(vmem_limit_bytes=32 * 1024 * 1024),
    )(*tables, qn, *kv_parts)


def step(queries, keys, values, next_latent, clip_blocks, valid_counts, group_ids, rewards):
    devices = lax.axis_size("tok")
    own_index = lax.axis_index("tok")
    _, width = queries.shape[1:]
    share = width // LEVEL
    levels = [list(range(first, first + LEVEL)) for first in range(0, devices, LEVEL)]
    heads = share // HEAD
    cuts = [0]
    for part in CHUNKS:
        cuts.append(cuts[-1] + heads * part // sum(CHUNKS))
    spans = [(low * HEAD, high * HEAD) for low, high in zip(cuts[:-1], cuts[1:])]

    def exchange(value):
        return lax.all_to_all(value, "tok", 0, 0, axis_index_groups=levels, tiled=True)

    def exchanged(value):
        found = exchange(value)
        return found.reshape(found.shape[0] * found.shape[1], found.shape[2])

    def gathered(own):
        found = [(REACH, LEVEL, own)]
        upward = downward = own
        held = LEVEL
        for distance in range(1, -(-REACH // LEVEL) + 1):
            count = min(LEVEL, REACH - (distance - 1) * LEVEL)
            upward = passed_along(upward[(held - count) * BLK :], "tok", LEVEL)
            downward = passed_along(downward[: count * BLK], "tok", -LEVEL)
            held = count
            found.append((max(0, REACH - distance * LEVEL), count, upward))
            found.append((REACH + distance * LEVEL, count, downward))
        return found

    own_kv = []
    for low, high in spans:
        part = packed(keys, values, low, high)
        own_kv.append(exchanged(part))
    part = packed(queries, next_latent, 0, share)
    qn = exchanged(part)

    valid_row = valid_counts[0]
    clip_row = clip_blocks[0]
    ends = jnp.cumsum(clip_row)
    starts = ends - clip_row
    positions = jnp.arange(valid_row.shape[0], dtype=jnp.int32)
    member = (starts[None, :] <= positions[:, None]) & (positions[:, None] < ends[None, :])
    tokens_of = jnp.sum(jnp.where(member, valid_row[:, None], 0), axis=0).astype(jnp.float32)
    clip_weight = advantages(rewards[0], group_ids[0]) / (2.0 * width * tokens_of)
    level_first = own_index // LEVEL * LEVEL
    own_ids = level_first + jnp.arange(LEVEL, dtype=jnp.int32)
    own_member = (starts[None, :] <= own_ids[:, None]) & (own_ids[:, None] < ends[None, :])
    own_weight = jnp.sum(jnp.where(own_member, clip_weight[None, :], 0.0), axis=1)
    place = jnp.stack([level_first, own_index - level_first])
    tables = (place, clip_blocks, valid_counts, own_weight)

    outs, errs = [], []
    for (low, high), own in zip(spans, own_kv):
        found = gathered(own)
        pieces = tuple((first, count) for first, count, _ in found)
        *out, err = attend(pieces, low // HEAD, tables, qn, [piece for _, _, piece in found])
        outs.append(out[0])
        for step in range(1, LEVEL):
            partners = [(source, source ^ step) for source in range(devices)]
            outs.append(lax.ppermute(out[step], "tok", partners))
        errs.append(err)
    velocity = unpacked(place, outs, spans, width)
    device_share = jnp.sum(sum(errs))
    everyone = devices * lax.axis_size("grp")
    spread = jnp.full((everyone, HEAD), device_share)
    total = jnp.sum(lax.all_to_all(spread, ("tok", "grp"), 0, 0, tiled=True)[:, 0])
    return (velocity, total)


def solution(mesh):
    return jax.shard_map(
        step,
        mesh=mesh,
        in_specs=(
            P("grp", "tok", None),
            P("grp", "tok", None),
            P("grp", "tok", None),
            P("grp", "tok", None),
            P("grp", None),
            P("grp", None),
            P("grp", None),
            P("grp", None),
        ),
        out_specs=(P("grp", "tok", None), P()),
        check_vma=False,
    )
```

```python
import functools
import math

import jax
import jax.numpy as jnp
from jax import lax
from jax.experimental import pallas as pl
from jax.experimental.pallas import tpu as pltpu
from jax.sharding import PartitionSpec as P


HEAD = 128
BLK = 128
MAXB = 8
GROUPS = 4
LEVEL = MAXB // 2
REACH = MAXB - 1
CHUNKS = (1, 1, 1)


masked_score = -1e30


def level_swap(value, axis, odd):
    count = lax.axis_size(axis)
    partners = [
        (source, ((source // LEVEL + odd) ^ 1) * LEVEL - odd * LEVEL + source % LEVEL)
        for source in range(count)
    ]
    return lax.ppermute(value, axis, [pair for pair in partners if 0 <= pair[1] < count])


def advantages(reward_row, group_row):
    member = (group_row[:, None] == jnp.arange(GROUPS, dtype=jnp.int32)[None, :]).astype(
        jnp.float32
    )
    totals = jnp.sum(member * reward_row[:, None], axis=0)
    counts = jnp.sum(member, axis=0)
    means = totals / jnp.maximum(counts, 1.0)
    return reward_row - jnp.sum(member * means[None, :], axis=1)


def moved(copies):
    for copy in copies:
        copy.start()
    for copy in copies:
        copy.wait()


def pack_body(spans, place_ref, first_ref, second_ref, *refs):
    out_refs, sems = refs[:-1], refs[-1]
    share = first_ref.shape[2] // LEVEL
    copies = []
    for index, out_ref in enumerate(out_refs):
        low, high = spans[index // LEVEL]
        span = high - low
        first = jnp.bitwise_xor(place_ref[1], index % LEVEL) * share + low
        for side, ref in enumerate((first_ref, second_ref)):
            copies.append(
                pltpu.make_async_copy(
                    ref.at[0, :, pl.ds(pl.multiple_of(first, HEAD), span)],
                    out_ref.at[:, pl.ds(side * span, span)],
                    sems.at[len(copies)],
                )
            )
    moved(copies)


def packed(place, first, second, spans):
    hbm = pl.BlockSpec(memory_space=pl.ANY)
    shapes = [
        jax.ShapeDtypeStruct((first.shape[1], 2 * (high - low)), first.dtype)
        for low, high in spans
        for _ in range(LEVEL)
    ]
    found = pl.pallas_call(
        functools.partial(pack_body, spans),
        out_shape=shapes,
        in_specs=[pl.BlockSpec(memory_space=pltpu.SMEM), hbm, hbm],
        out_specs=[pl.BlockSpec(memory_space=pltpu.VMEM)] * len(shapes),
        scratch_shapes=[pltpu.SemaphoreType.DMA((2 * len(shapes),))],
    )(place, first, second)
    return [found[first : first + LEVEL] for first in range(0, len(shapes), LEVEL)]


def join_body(place_ref, *refs):
    for step, ref in enumerate(refs[:-1]):
        first = jnp.bitwise_xor(place_ref[1], step) * BLK
        refs[-1][pl.ds(pl.multiple_of(first, BLK), BLK), :] = ref[...]


def joined(place, parts):
    vmem = pl.BlockSpec(memory_space=pltpu.VMEM)
    rows, width = parts[0].shape
    return pl.pallas_call(
        join_body,
        out_shape=jax.ShapeDtypeStruct((len(parts) * rows, width), parts[0].dtype),
        in_specs=[pl.BlockSpec(memory_space=pltpu.SMEM)] + [vmem] * len(parts),
        out_specs=vmem,
    )(place, *parts)


def unpack_body(spans, place_ref, *refs):
    parts, out_ref = refs[:-1], refs[-1]
    share = out_ref.shape[2] // LEVEL
    for index, (low, high) in enumerate(spans):
        for step in range(LEVEL):
            first = pl.multiple_of(jnp.bitwise_xor(place_ref[1], step) * share + low, HEAD)
            out_ref[0, :, pl.ds(first, high - low)] = parts[index * LEVEL + step][...]


def unpacked(place, outs, spans, width):
    vmem = pl.BlockSpec(memory_space=pltpu.VMEM)
    return pl.pallas_call(
        functools.partial(unpack_body, spans),
        out_shape=jax.ShapeDtypeStruct((1, outs[0].shape[0], width), outs[0].dtype),
        in_specs=[pl.BlockSpec(memory_space=pltpu.SMEM)] + [vmem] * len(outs),
        out_specs=vmem,
        name="unpack",
    )(place, *outs)


def kernel_body(heads, first_head, earlier, place_ref, clip_ref, valid_ref, weight_ref, *refs):
    earlier, refs = refs[:earlier], refs[earlier:]
    width = heads * HEAD
    qn_ref, kv_parts = refs[0], refs[1:6]
    out_refs = refs[6 : 6 + LEVEL]
    err_ref, kv_buf = refs[6 + LEVEL :]
    half = qn_ref.shape[1] // 2
    level_first, own, odd = place_ref[0], place_ref[1], place_ref[2]
    sides = (REACH + LEVEL, REACH - LEVEL)
    ends = (REACH + 2 * LEVEL, 0)
    firsts = [
        jnp.int32(REACH),
        jnp.where(odd == 0, *sides),
        jnp.where(odd == 1, *sides),
        jnp.where(odd == 0, *ends),
        jnp.where(odd == 1, *ends),
    ]
    err = jnp.zeros((8, HEAD), jnp.float32)
    for ref in earlier:
        err = err + ref[...]
    factor = math.log2(math.e) / math.sqrt(HEAD)
    last_block = valid_ref.shape[1] - 1
    slots = lax.broadcasted_iota(jnp.int32, (1, BLK), 1)
    blocks = []
    for step in range(LEVEL):
        block = jnp.bitwise_xor(own, step)
        own_id = level_first + block
        clip_start = clip_count = clip_first = jnp.int32(0)
        for clip in range(clip_ref.shape[1]):
            count = clip_ref[0, clip]
            mine = (own_id >= clip_first) & (own_id < clip_first + count)
            clip_start = jnp.where(mine, clip_first, clip_start)
            clip_count = jnp.where(mine, count, clip_count)
            clip_first = clip_first + count
        bias = []
        for near in range(MAXB):
            live = valid_ref[0, jnp.minimum(clip_start + near, last_block)]
            live = jnp.where(near < clip_count, live, 0)
            bias.append(jnp.where(slots < live, 0.0, masked_score).astype(jnp.float32))
        window_first = clip_start - (level_first - REACH)
        blocks.append(
            (
                pl.ds(pl.multiple_of(block * BLK, BLK), BLK),
                pl.ds(pl.multiple_of(window_first * BLK, BLK), MAXB * BLK),
                jnp.concatenate(bias, axis=1),
                valid_ref[0, own_id],
                weight_ref[block],
            )
        )
    for head in range(heads):
        columns = slice(head * HEAD, (head + 1) * HEAD)
        other = slice(width + head * HEAD, width + (head + 1) * HEAD)
        own_columns = slice((first_head + head) * HEAD, (first_head + head + 1) * HEAD)
        own_other = slice(half + own_columns.start, half + own_columns.stop)
        for ref, first in zip(kv_parts, firsts):
            rows = pl.ds(pl.multiple_of(first * BLK, BLK), ref.shape[0])
            kv_buf[rows, columns] = ref[:, columns]
            kv_buf[rows, other] = ref[:, other]
        for step, (rows, window, bias, live, weight) in enumerate(blocks):
            scores = lax.dot_general(
                qn_ref[rows, own_columns],
                kv_buf[window, columns],
                (((1,), (1,)), ((), ())),
                preferred_element_type=jnp.float32,
            )
            scores = scores + bias
            top = jnp.max(scores, axis=-1, keepdims=True)
            expo = jnp.exp2((scores - top) * factor)
            probs = (expo * (1.0 / jnp.sum(expo, axis=-1, keepdims=True))).astype(jnp.bfloat16)
            mixed = lax.dot_general(
                probs,
                kv_buf[window, other],
                (((1,), (0,)), ((), ())),
                preferred_element_type=jnp.float32,
            )
            own_live = lax.broadcasted_iota(jnp.int32, (BLK, HEAD), 0) < live
            result = jnp.where(own_live, mixed, 0.0).astype(jnp.bfloat16)
            out_refs[step][:, columns] = result
            diff = qn_ref[rows, own_other].astype(jnp.float32) - result.astype(jnp.float32)
            block_err = jnp.where(own_live, diff * diff, 0.0)
            err = err + weight * jnp.sum(block_err.reshape(BLK // 8, 8, HEAD), axis=0)
    if err_ref.shape[0] != err.shape[0]:
        err = jnp.broadcast_to(jnp.sum(err, keepdims=True), err_ref.shape)
    err_ref[...] = err


def attend(first_head, tables, earlier, spread, qn, kv_parts):
    width = kv_parts[0].shape[1] // 2
    heads = width // HEAD
    total = sum(part.shape[0] for part in kv_parts)
    smem = pl.BlockSpec(memory_space=pltpu.SMEM)
    vmem = pl.BlockSpec(memory_space=pltpu.VMEM)
    units = LEVEL * heads
    return pl.pallas_call(
        functools.partial(kernel_body, heads, first_head, len(earlier)),
        out_shape=[jax.ShapeDtypeStruct((BLK, width), jnp.bfloat16)] * LEVEL
        + [jax.ShapeDtypeStruct((spread, HEAD), jnp.float32)],
        in_specs=[smem] * len(tables) + [vmem] * (len(earlier) + 1 + len(kv_parts)),
        out_specs=[vmem] * (LEVEL + 1),
        scratch_shapes=[
            pltpu.VMEM((total, 2 * width), jnp.bfloat16),
        ],
        cost_estimate=pl.CostEstimate(
            flops=units * 4 * BLK * MAXB * BLK * HEAD,
            transcendentals=units * BLK * MAXB * BLK,
            bytes_accessed=4 * (total + 2 * qn.shape[0]) * width,
        ),
        compiler_params=pltpu.CompilerParams(vmem_limit_bytes=24 * 1024 * 1024),
    )(*tables, *earlier, qn, *kv_parts)


def step(queries, keys, values, next_latent, clip_blocks, valid_counts, group_ids, rewards):
    devices = lax.axis_size("tok")
    own_index = lax.axis_index("tok")
    _, width = queries.shape[1:]
    share = width // LEVEL
    heads = share // HEAD
    cuts = [0]
    for part in CHUNKS:
        cuts.append(cuts[-1] + heads * part // sum(CHUNKS))
    spans = [(low * HEAD, high * HEAD) for low, high in zip(cuts[:-1], cuts[1:])]

    def swapped(parts):
        found = [parts[0]]
        for step in range(1, LEVEL):
            partners = [(source, source ^ step) for source in range(devices)]
            found.append(lax.ppermute(parts[step], "tok", partners))
        return found

    level = own_index // LEVEL
    level_first = level * LEVEL
    odd = level % 2
    place = jnp.stack([level_first, own_index - level_first, odd])

    def gathered(own):
        reached = (REACH - LEVEL) * BLK
        upper = LEVEL * BLK - reached
        first = [level_swap(own, "tok", side) for side in (0, 1)]
        starts = (jnp.where(odd == 0, upper, 0), jnp.where(odd == 1, upper, 0))
        second = [
            level_swap(lax.dynamic_slice_in_dim(value, start, reached, 0), "tok", side)
            for side, (value, start) in enumerate(zip(first[::-1], starts))
        ]
        return [own, *first, *second]

    own_kv = []
    packs = packed(place, keys, values, spans[:1])
    packs += packed(place, keys, values, spans[1:])
    for parts in packs:
        parts = swapped(parts)
        own_kv.append(joined(place, parts))
    (parts,) = packed(place, queries, next_latent, [(0, share)])
    parts = swapped(parts)
    qn = joined(place, parts)

    valid_row = valid_counts[0]
    clip_row = clip_blocks[0]
    ends = jnp.cumsum(clip_row)
    starts = ends - clip_row
    positions = jnp.arange(valid_row.shape[0], dtype=jnp.int32)
    member = (starts[None, :] <= positions[:, None]) & (positions[:, None] < ends[None, :])
    tokens_of = jnp.sum(jnp.where(member, valid_row[:, None], 0), axis=0).astype(jnp.float32)
    clip_weight = advantages(rewards[0], group_ids[0]) / (2.0 * width * tokens_of)
    own_ids = level_first + jnp.arange(LEVEL, dtype=jnp.int32)
    own_member = (starts[None, :] <= own_ids[:, None]) & (own_ids[:, None] < ends[None, :])
    own_weight = jnp.sum(jnp.where(own_member, clip_weight[None, :], 0.0), axis=1)
    tables = (place, clip_blocks, valid_counts, own_weight)

    everyone = devices * lax.axis_size("grp")
    outs, errs = [], []
    for index, ((low, high), own) in enumerate(zip(spans, own_kv)):
        found = gathered(own)
        *out, err = attend(
            low // HEAD, tables, errs[-1:], everyone if index == len(spans) - 1 else 8, qn, found
        )
        outs += swapped(out)
        errs.append(err)
    velocity = unpacked(place, outs, spans, width)
    total = jnp.sum(lax.all_to_all(errs[-1], ("tok", "grp"), 0, 0, tiled=True)[:, 0])
    return (velocity, total)


def solution(mesh):
    return jax.shard_map(
        step,
        mesh=mesh,
        in_specs=(
            P("grp", "tok", None),
            P("grp", "tok", None),
            P("grp", "tok", None),
            P("grp", "tok", None),
            P("grp", None),
            P("grp", None),
            P("grp", None),
            P("grp", None),
        ),
        out_specs=(P("grp", "tok", None), P()),
        check_vma=False,
    )
```

```python
import functools
import math

import jax
import jax.numpy as jnp
from jax import lax
from jax.experimental import pallas as pl
from jax.experimental.pallas import tpu as pltpu
from jax.sharding import PartitionSpec as P


HEAD = 128
BLK = 128
MAXB = 8
GROUPS = 4
LEVEL = MAXB // 2
REACH = MAXB - 1
CHUNKS = (1, 1, 1)


masked_score = -1e30
small_grant = pltpu.CompilerParams(vmem_limit_bytes=6 * 1024 * 1024)


def level_swap(value, axis, odd):
    count = lax.axis_size(axis)
    partners = [
        (source, ((source // LEVEL + odd) ^ 1) * LEVEL - odd * LEVEL + source % LEVEL)
        for source in range(count)
    ]
    return lax.ppermute(value, axis, [pair for pair in partners if 0 <= pair[1] < count])


def advantages(reward_row, group_row):
    member = (group_row[:, None] == jnp.arange(GROUPS, dtype=jnp.int32)[None, :]).astype(
        jnp.float32
    )
    totals = jnp.sum(member * reward_row[:, None], axis=0)
    counts = jnp.sum(member, axis=0)
    means = totals / jnp.maximum(counts, 1.0)
    return reward_row - jnp.sum(member * means[None, :], axis=1)


def moved(copies):
    for copy in copies:
        copy.start()
    for copy in copies:
        copy.wait()


def pack_body(spans, place_ref, first_ref, second_ref, *refs):
    out_refs, sems = refs[:-1], refs[-1]
    share = first_ref.shape[2] // LEVEL
    copies = []
    for index, out_ref in enumerate(out_refs):
        low, high = spans[index // LEVEL]
        span = high - low
        first = jnp.bitwise_xor(place_ref[1], index % LEVEL) * share + low
        for side, ref in enumerate((first_ref, second_ref)):
            copies.append(
                pltpu.make_async_copy(
                    ref.at[0, :, pl.ds(pl.multiple_of(first, HEAD), span)],
                    out_ref.at[:, pl.ds(side * span, span)],
                    sems.at[len(copies)],
                )
            )
    moved(copies)


def packed(place, first, second, spans):
    hbm = pl.BlockSpec(memory_space=pl.ANY)
    shapes = [
        jax.ShapeDtypeStruct((first.shape[1], 2 * (high - low)), first.dtype)
        for low, high in spans
        for _ in range(LEVEL)
    ]
    found = pl.pallas_call(
        functools.partial(pack_body, spans),
        out_shape=shapes,
        in_specs=[pl.BlockSpec(memory_space=pltpu.SMEM), hbm, hbm],
        out_specs=[pl.BlockSpec(memory_space=pltpu.VMEM)] * len(shapes),
        scratch_shapes=[pltpu.SemaphoreType.DMA((2 * len(shapes),))],
        compiler_params=small_grant,
    )(place, first, second)
    return [found[first : first + LEVEL] for first in range(0, len(shapes), LEVEL)]


def join_body(place_ref, *refs):
    for step, ref in enumerate(refs[:-1]):
        first = jnp.bitwise_xor(place_ref[1], step) * BLK
        refs[-1][pl.ds(pl.multiple_of(first, BLK), BLK), :] = ref[...]


def joined(place, parts):
    vmem = pl.BlockSpec(memory_space=pltpu.VMEM)
    rows, width = parts[0].shape
    return pl.pallas_call(
        join_body,
        out_shape=jax.ShapeDtypeStruct((len(parts) * rows, width), parts[0].dtype),
        in_specs=[pl.BlockSpec(memory_space=pltpu.SMEM)] + [vmem] * len(parts),
        out_specs=vmem,
        compiler_params=small_grant,
    )(place, *parts)


def unpack_body(spans, place_ref, *refs):
    parts, out_ref = refs[:-1], refs[-1]
    share = out_ref.shape[2] // LEVEL
    for index, (low, high) in enumerate(spans):
        for step in range(LEVEL):
            first = pl.multiple_of(jnp.bitwise_xor(place_ref[1], step) * share + low, HEAD)
            out_ref[0, :, pl.ds(first, high - low)] = parts[index * LEVEL + step][...]


def unpacked(place, outs, spans, width):
    vmem = pl.BlockSpec(memory_space=pltpu.VMEM)
    return pl.pallas_call(
        functools.partial(unpack_body, spans),
        out_shape=jax.ShapeDtypeStruct((1, outs[0].shape[0], width), outs[0].dtype),
        in_specs=[pl.BlockSpec(memory_space=pltpu.SMEM)] + [vmem] * len(outs),
        out_specs=vmem,
        compiler_params=small_grant,
        name="unpack",
    )(place, *outs)


def kernel_body(heads, first_head, earlier, place_ref, clip_ref, valid_ref, weight_ref, *refs):
    earlier, refs = refs[:earlier], refs[earlier:]
    width = heads * HEAD
    qn_refs, kv_parts = refs[:LEVEL], refs[LEVEL : LEVEL + 5]
    out_refs = refs[LEVEL + 5 : 2 * LEVEL + 5]
    err_ref, kv_buf = refs[2 * LEVEL + 5 :]
    half = qn_refs[0].shape[1] // 2
    level_first, own, odd = place_ref[0], place_ref[1], place_ref[2]
    sides = (REACH + LEVEL, REACH - LEVEL)
    ends = (REACH + 2 * LEVEL, 0)
    firsts = [
        jnp.int32(REACH),
        jnp.where(odd == 0, *sides),
        jnp.where(odd == 1, *sides),
        jnp.where(odd == 0, *ends),
        jnp.where(odd == 1, *ends),
    ]
    err = jnp.zeros((8, HEAD), jnp.float32)
    for ref in earlier:
        err = err + ref[...]
    factor = math.log2(math.e) / math.sqrt(HEAD)
    last_block = valid_ref.shape[1] - 1
    slots = lax.broadcasted_iota(jnp.int32, (1, BLK), 1)
    blocks = []
    for step in range(LEVEL):
        block = jnp.bitwise_xor(own, step)
        own_id = level_first + block
        clip_start = clip_count = clip_first = jnp.int32(0)
        for clip in range(clip_ref.shape[1]):
            count = clip_ref[0, clip]
            mine = (own_id >= clip_first) & (own_id < clip_first + count)
            clip_start = jnp.where(mine, clip_first, clip_start)
            clip_count = jnp.where(mine, count, clip_count)
            clip_first = clip_first + count
        bias = []
        for near in range(MAXB):
            live = valid_ref[0, jnp.minimum(clip_start + near, last_block)]
            live = jnp.where(near < clip_count, live, 0)
            bias.append(jnp.where(slots < live, 0.0, masked_score).astype(jnp.float32))
        window_first = clip_start - (level_first - REACH)
        blocks.append(
            (
                pl.ds(pl.multiple_of(window_first * BLK, BLK), MAXB * BLK),
                jnp.concatenate(bias, axis=1),
                valid_ref[0, own_id],
                weight_ref[block],
            )
        )
    for head in range(heads):
        columns = slice(head * HEAD, (head + 1) * HEAD)
        other = slice(width + head * HEAD, width + (head + 1) * HEAD)
        own_columns = slice((first_head + head) * HEAD, (first_head + head + 1) * HEAD)
        own_other = slice(half + own_columns.start, half + own_columns.stop)
        for ref, first in zip(kv_parts, firsts):
            rows = pl.ds(pl.multiple_of(first * BLK, BLK), ref.shape[0])
            kv_buf[rows, columns] = ref[:, columns]
            kv_buf[rows, other] = ref[:, other]
        for step, (window, bias, live, weight) in enumerate(blocks):
            scores = lax.dot_general(
                qn_refs[step][:, own_columns],
                kv_buf[window, columns],
                (((1,), (1,)), ((), ())),
                preferred_element_type=jnp.float32,
            )
            scores = scores + bias
            top = jnp.max(scores, axis=-1, keepdims=True)
            expo = jnp.exp2((scores - top) * factor)
            probs = (expo * (1.0 / jnp.sum(expo, axis=-1, keepdims=True))).astype(jnp.bfloat16)
            mixed = lax.dot_general(
                probs,
                kv_buf[window, other],
                (((1,), (0,)), ((), ())),
                preferred_element_type=jnp.float32,
            )
            own_live = lax.broadcasted_iota(jnp.int32, (BLK, HEAD), 0) < live
            result = jnp.where(own_live, mixed, 0.0).astype(jnp.bfloat16)
            out_refs[step][:, columns] = result
            diff = qn_refs[step][:, own_other].astype(jnp.float32) - result.astype(jnp.float32)
            block_err = jnp.where(own_live, diff * diff, 0.0)
            err = err + weight * jnp.sum(block_err.reshape(BLK // 8, 8, HEAD), axis=0)
    if err_ref.shape[0] != err.shape[0]:
        err = jnp.broadcast_to(jnp.sum(err, keepdims=True), err_ref.shape)
    err_ref[...] = err


def attend(first_head, tables, earlier, spread, qn, kv_parts):
    width = kv_parts[0].shape[1] // 2
    heads = width // HEAD
    total = sum(part.shape[0] for part in kv_parts)
    smem = pl.BlockSpec(memory_space=pltpu.SMEM)
    vmem = pl.BlockSpec(memory_space=pltpu.VMEM)
    units = LEVEL * heads
    return pl.pallas_call(
        functools.partial(kernel_body, heads, first_head, len(earlier)),
        out_shape=[jax.ShapeDtypeStruct((BLK, width), jnp.bfloat16)] * LEVEL
        + [jax.ShapeDtypeStruct((spread, HEAD), jnp.float32)],
        in_specs=[smem] * len(tables) + [vmem] * (len(earlier) + len(qn) + len(kv_parts)),
        out_specs=[vmem] * (LEVEL + 1),
        scratch_shapes=[
            pltpu.VMEM((total, 2 * width), jnp.bfloat16),
        ],
        cost_estimate=pl.CostEstimate(
            flops=units * 4 * BLK * MAXB * BLK * HEAD,
            transcendentals=units * BLK * MAXB * BLK,
            bytes_accessed=4 * (total + 2 * LEVEL * BLK) * width,
        ),
        compiler_params=pltpu.CompilerParams(vmem_limit_bytes=12 * 1024 * 1024),
    )(*tables, *earlier, *qn, *kv_parts)


def step(queries, keys, values, next_latent, clip_blocks, valid_counts, group_ids, rewards):
    devices = lax.axis_size("tok")
    own_index = lax.axis_index("tok")
    _, width = queries.shape[1:]
    share = width // LEVEL
    heads = share // HEAD
    cuts = [0]
    for part in CHUNKS:
        cuts.append(cuts[-1] + heads * part // sum(CHUNKS))
    spans = [(low * HEAD, high * HEAD) for low, high in zip(cuts[:-1], cuts[1:])]

    def swapped(parts):
        found = [parts[0]]
        for step in range(1, LEVEL):
            partners = [(source, source ^ step) for source in range(devices)]
            found.append(lax.ppermute(parts[step], "tok", partners))
        return found

    level = own_index // LEVEL
    level_first = level * LEVEL
    odd = level % 2
    place = jnp.stack([level_first, own_index - level_first, odd])

    def gathered(own):
        reached = (REACH - LEVEL) * BLK
        upper = LEVEL * BLK - reached
        first, second = [], []
        for side in (0, 1):
            first.append(level_swap(own, "tok", side))
        for side in (0, 1):
            start = jnp.where(odd == side, upper, 0)
            passed = lax.dynamic_slice_in_dim(first[1 - side], start, reached, 0)
            second.append(level_swap(passed, "tok", side))
        return [own, *first, *second]

    own_kv = []
    packs = packed(place, keys, values, spans[:1])
    packs += packed(place, keys, values, spans[1:])
    for parts in packs:
        parts = swapped(parts)
        own_kv.append(joined(place, parts))
    (parts,) = packed(place, queries, next_latent, [(0, share)])
    qn = swapped(parts)

    valid_row = valid_counts[0]
    clip_row = clip_blocks[0]
    ends = jnp.cumsum(clip_row)
    starts = ends - clip_row
    positions = jnp.arange(valid_row.shape[0], dtype=jnp.int32)
    member = (starts[None, :] <= positions[:, None]) & (positions[:, None] < ends[None, :])
    tokens_of = jnp.sum(jnp.where(member, valid_row[:, None], 0), axis=0).astype(jnp.float32)
    clip_weight = advantages(rewards[0], group_ids[0]) / (2.0 * width * tokens_of)
    own_ids = level_first + jnp.arange(LEVEL, dtype=jnp.int32)
    own_member = (starts[None, :] <= own_ids[:, None]) & (own_ids[:, None] < ends[None, :])
    own_weight = jnp.sum(jnp.where(own_member, clip_weight[None, :], 0.0), axis=1)
    tables = (place, clip_blocks, valid_counts, own_weight)

    everyone = devices * lax.axis_size("grp")
    outs, errs = [], []
    for index, ((low, high), own) in enumerate(zip(spans, own_kv)):
        found = gathered(own)
        *out, err = attend(
            low // HEAD, tables, errs[-1:], everyone if index == len(spans) - 1 else 8, qn, found
        )
        outs += swapped(out)
        errs.append(err)
    velocity = unpacked(place, outs, spans, width)
    total = jnp.sum(lax.all_to_all(errs[-1], ("tok", "grp"), 0, 0, tiled=True)[:, 0])
    return (velocity, total)


def solution(mesh):
    return jax.shard_map(
        step,
        mesh=mesh,
        in_specs=(
            P("grp", "tok", None),
            P("grp", "tok", None),
            P("grp", "tok", None),
            P("grp", "tok", None),
            P("grp", None),
            P("grp", None),
            P("grp", None),
            P("grp", None),
        ),
        out_specs=(P("grp", "tok", None), P()),
        check_vma=False,
    )
```

```python
import functools
import math

import jax
import jax.numpy as jnp
from jax import lax
from jax.experimental import pallas as pl
from jax.experimental.pallas import tpu as pltpu
from jax.sharding import PartitionSpec as P


HEAD = 128
BLK = 128
MAXB = 8
GROUPS = 4
LEVEL = MAXB // 2
REACH = MAXB - 1
CHUNKS = (1, 2, 2, 1)


masked_score = -1e30
small_grant = pltpu.CompilerParams(vmem_limit_bytes=6 * 1024 * 1024)


def level_swap(value, axis, odd):
    count = lax.axis_size(axis)
    partners = [
        (source, ((source // LEVEL + odd) ^ 1) * LEVEL - odd * LEVEL + source % LEVEL)
        for source in range(count)
    ]
    return lax.ppermute(value, axis, [pair for pair in partners if 0 <= pair[1] < count])


def advantages(reward_row, group_row):
    member = (group_row[:, None] == jnp.arange(GROUPS, dtype=jnp.int32)[None, :]).astype(
        jnp.float32
    )
    totals = jnp.sum(member * reward_row[:, None], axis=0)
    counts = jnp.sum(member, axis=0)
    means = totals / jnp.maximum(counts, 1.0)
    return reward_row - jnp.sum(member * means[None, :], axis=1)


def moved(copies):
    for copy in copies:
        copy.start()
    for copy in copies:
        copy.wait()


def pack_body(spans, place_ref, first_ref, second_ref, *refs):
    out_refs, sems = refs[:-1], refs[-1]
    share = first_ref.shape[2] // LEVEL
    copies = []
    for index, out_ref in enumerate(out_refs):
        low, high = spans[index // LEVEL]
        span = high - low
        first = jnp.bitwise_xor(place_ref[1], index % LEVEL) * share + low
        for side, ref in enumerate((first_ref, second_ref)):
            copies.append(
                pltpu.make_async_copy(
                    ref.at[0, :, pl.ds(pl.multiple_of(first, HEAD), span)],
                    out_ref.at[:, pl.ds(side * span, span)],
                    sems.at[len(copies)],
                )
            )
    moved(copies)


def packed(place, first, second, spans):
    hbm = pl.BlockSpec(memory_space=pltpu.HBM)
    shapes = [
        jax.ShapeDtypeStruct((first.shape[1], 2 * (high - low)), first.dtype)
        for low, high in spans
        for _ in range(LEVEL)
    ]
    found = pl.pallas_call(
        functools.partial(pack_body, spans),
        out_shape=shapes,
        in_specs=[pl.BlockSpec(memory_space=pltpu.SMEM), hbm, hbm],
        out_specs=[pl.BlockSpec(memory_space=pltpu.VMEM)] * len(shapes),
        scratch_shapes=[pltpu.SemaphoreType.DMA((2 * len(shapes),))],
        compiler_params=small_grant,
    )(place, first, second)
    return [found[first : first + LEVEL] for first in range(0, len(shapes), LEVEL)]


def join_body(place_ref, *refs):
    for step, ref in enumerate(refs[:-1]):
        first = jnp.bitwise_xor(place_ref[1], step) * BLK
        refs[-1][pl.ds(pl.multiple_of(first, BLK), BLK), :] = ref[...]


def joined(place, parts):
    vmem = pl.BlockSpec(memory_space=pltpu.VMEM)
    rows, width = parts[0].shape
    return pl.pallas_call(
        join_body,
        out_shape=jax.ShapeDtypeStruct((len(parts) * rows, width), parts[0].dtype),
        in_specs=[pl.BlockSpec(memory_space=pltpu.SMEM)] + [vmem] * len(parts),
        out_specs=vmem,
        compiler_params=small_grant,
    )(place, *parts)


def unpack_body(spans, place_ref, *refs):
    parts, out_ref = refs[:-1], refs[-1]
    share = out_ref.shape[2] // LEVEL
    for index, (low, high) in enumerate(spans):
        for step in range(LEVEL):
            first = pl.multiple_of(jnp.bitwise_xor(place_ref[1], step) * share + low, HEAD)
            out_ref[0, :, pl.ds(first, high - low)] = parts[index * LEVEL + step][...]


def unpacked(place, outs, spans, width):
    vmem = pl.BlockSpec(memory_space=pltpu.VMEM)
    return pl.pallas_call(
        functools.partial(unpack_body, spans),
        out_shape=jax.ShapeDtypeStruct((1, outs[0].shape[0], width), outs[0].dtype),
        in_specs=[pl.BlockSpec(memory_space=pltpu.SMEM)] + [vmem] * len(outs),
        out_specs=vmem,
        compiler_params=small_grant,
        name="unpack",
    )(place, *outs)


def kernel_body(heads, first_head, earlier, place_ref, clip_ref, valid_ref, weight_ref, *refs):
    earlier, refs = refs[:earlier], refs[earlier:]
    width = heads * HEAD
    qn_refs, kv_parts = refs[:LEVEL], refs[LEVEL : LEVEL + 5]
    out_refs = refs[LEVEL + 5 : 2 * LEVEL + 5]
    err_ref, kv_buf = refs[2 * LEVEL + 5 :]
    half = qn_refs[0].shape[1] // 2
    level_first, own, odd = place_ref[0], place_ref[1], place_ref[2]
    sides = (REACH + LEVEL, REACH - LEVEL)
    ends = (REACH + 2 * LEVEL, 0)
    firsts = [
        jnp.int32(REACH),
        jnp.where(odd == 0, *sides),
        jnp.where(odd == 1, *sides),
        jnp.where(odd == 0, *ends),
        jnp.where(odd == 1, *ends),
    ]
    err = jnp.zeros((8, HEAD), jnp.float32)
    for ref in earlier:
        err = err + ref[...]
    factor = math.log2(math.e) / math.sqrt(HEAD)
    last_block = valid_ref.shape[1] - 1
    slots = lax.broadcasted_iota(jnp.int32, (1, BLK), 1)
    blocks = []
    for step in range(LEVEL):
        block = jnp.bitwise_xor(own, step)
        own_id = level_first + block
        clip_start = clip_count = clip_first = jnp.int32(0)
        for clip in range(clip_ref.shape[1]):
            count = clip_ref[0, clip]
            mine = (own_id >= clip_first) & (own_id < clip_first + count)
            clip_start = jnp.where(mine, clip_first, clip_start)
            clip_count = jnp.where(mine, count, clip_count)
            clip_first = clip_first + count
        bias = []
        for near in range(MAXB):
            live = valid_ref[0, jnp.minimum(clip_start + near, last_block)]
            live = jnp.where(near < clip_count, live, 0)
            bias.append(jnp.where(slots < live, 0.0, masked_score).astype(jnp.float32))
        window_first = clip_start - (level_first - REACH)
        blocks.append(
            (
                pl.ds(pl.multiple_of(window_first * BLK, BLK), MAXB * BLK),
                jnp.concatenate(bias, axis=1),
                valid_ref[0, own_id],
                weight_ref[block],
            )
        )
    for head in range(heads):
        columns = slice(head * HEAD, (head + 1) * HEAD)
        other = slice(width + head * HEAD, width + (head + 1) * HEAD)
        own_columns = slice((first_head + head) * HEAD, (first_head + head + 1) * HEAD)
        own_other = slice(half + own_columns.start, half + own_columns.stop)
        for ref, first in zip(kv_parts, firsts):
            rows = pl.ds(pl.multiple_of(first * BLK, BLK), ref.shape[0])
            kv_buf[rows, columns] = ref[:, columns]
            kv_buf[rows, other] = ref[:, other]
        for step, (window, bias, live, weight) in enumerate(blocks):
            scores = lax.dot_general(
                qn_refs[step][:, own_columns],
                kv_buf[window, columns],
                (((1,), (1,)), ((), ())),
                preferred_element_type=jnp.float32,
            )
            scores = scores + bias
            top = jnp.max(scores, axis=-1, keepdims=True)
            expo = jnp.exp2((scores - top) * factor)
            probs = (expo * (1.0 / jnp.sum(expo, axis=-1, keepdims=True))).astype(jnp.bfloat16)
            mixed = lax.dot_general(
                probs,
                kv_buf[window, other],
                (((1,), (0,)), ((), ())),
                preferred_element_type=jnp.float32,
            )
            own_live = lax.broadcasted_iota(jnp.int32, (BLK, HEAD), 0) < live
            result = jnp.where(own_live, mixed, 0.0).astype(jnp.bfloat16)
            out_refs[step][:, columns] = result
            diff = qn_refs[step][:, own_other].astype(jnp.float32) - result.astype(jnp.float32)
            block_err = jnp.where(own_live, diff * diff, 0.0)
            err = err + weight * jnp.sum(block_err.reshape(BLK // 8, 8, HEAD), axis=0)
    if err_ref.shape[0] != err.shape[0]:
        err = jnp.broadcast_to(jnp.sum(err, keepdims=True), err_ref.shape)
    err_ref[...] = err


def attend(first_head, tables, earlier, spread, qn, kv_parts):
    width = kv_parts[0].shape[1] // 2
    heads = width // HEAD
    total = sum(part.shape[0] for part in kv_parts)
    smem = pl.BlockSpec(memory_space=pltpu.SMEM)
    vmem = pl.BlockSpec(memory_space=pltpu.VMEM)
    units = LEVEL * heads
    return pl.pallas_call(
        functools.partial(kernel_body, heads, first_head, len(earlier)),
        out_shape=[jax.ShapeDtypeStruct((BLK, width), jnp.bfloat16)] * LEVEL
        + [jax.ShapeDtypeStruct((spread, HEAD), jnp.float32)],
        in_specs=[smem] * len(tables) + [vmem] * (len(earlier) + len(qn) + len(kv_parts)),
        out_specs=[vmem] * (LEVEL + 1),
        scratch_shapes=[
            pltpu.VMEM((total, 2 * width), jnp.bfloat16),
        ],
        cost_estimate=pl.CostEstimate(
            flops=units * 4 * BLK * MAXB * BLK * HEAD,
            transcendentals=units * BLK * MAXB * BLK,
            bytes_accessed=4 * (total + 2 * LEVEL * BLK) * width,
        ),
        compiler_params=pltpu.CompilerParams(vmem_limit_bytes=12 * 1024 * 1024),
    )(*tables, *earlier, *qn, *kv_parts)


def step(queries, keys, values, next_latent, clip_blocks, valid_counts, group_ids, rewards):
    devices = lax.axis_size("tok")
    own_index = lax.axis_index("tok")
    _, width = queries.shape[1:]
    share = width // LEVEL
    heads = share // HEAD
    cuts = [0]
    for part in CHUNKS:
        cuts.append(cuts[-1] + heads * part // sum(CHUNKS))
    spans = [(low * HEAD, high * HEAD) for low, high in zip(cuts[:-1], cuts[1:])]

    def swapped(parts):
        found = [parts[0]]
        for step in range(1, LEVEL):
            partners = [(source, source ^ step) for source in range(devices)]
            found.append(lax.ppermute(parts[step], "tok", partners))
        return found

    level = own_index // LEVEL
    level_first = level * LEVEL
    odd = level % 2
    place = jnp.stack([level_first, own_index - level_first, odd])

    def gathered(own):
        reached = (REACH - LEVEL) * BLK
        upper = LEVEL * BLK - reached
        first, second = [], []
        for side in (0, 1):
            first.append(level_swap(own, "tok", side))
        for side in (0, 1):
            start = jnp.where(odd == side, upper, 0)
            passed = lax.dynamic_slice_in_dim(first[1 - side], start, reached, 0)
            second.append(level_swap(passed, "tok", side))
        return [own, *first, *second]

    own_kv = []
    in_hbm = [pltpu.with_memory_space_constraint(value, pltpu.HBM) for value in (keys, values)]
    packs = packed(place, *in_hbm, spans[:1])
    packs += packed(place, keys, values, spans[1:])
    for parts in packs:
        parts = swapped(parts)
        own_kv.append(joined(place, parts))
    (parts,) = packed(place, queries, next_latent, [(0, share)])
    qn = swapped(parts)

    valid_row = valid_counts[0]
    clip_row = clip_blocks[0]
    ends = jnp.cumsum(clip_row)
    starts = ends - clip_row
    positions = jnp.arange(valid_row.shape[0], dtype=jnp.int32)
    member = (starts[None, :] <= positions[:, None]) & (positions[:, None] < ends[None, :])
    tokens_of = jnp.sum(jnp.where(member, valid_row[:, None], 0), axis=0).astype(jnp.float32)
    clip_weight = advantages(rewards[0], group_ids[0]) / (2.0 * width * tokens_of)
    own_ids = level_first + jnp.arange(LEVEL, dtype=jnp.int32)
    own_member = (starts[None, :] <= own_ids[:, None]) & (own_ids[:, None] < ends[None, :])
    own_weight = jnp.sum(jnp.where(own_member, clip_weight[None, :], 0.0), axis=1)
    tables = (place, clip_blocks, valid_counts, own_weight)

    everyone = devices * lax.axis_size("grp")
    outs, errs = [], []
    for index, ((low, high), own) in enumerate(zip(spans, own_kv)):
        found = gathered(own)
        *out, err = attend(
            low // HEAD, tables, errs[-1:], everyone if index == len(spans) - 1 else 8, qn, found
        )
        outs += swapped(out)
        errs.append(err)
    velocity = unpacked(place, outs, spans, width)
    total = jnp.sum(lax.all_to_all(errs[-1], ("tok", "grp"), 0, 0, tiled=True)[:, 0])
    return (velocity, total)


def solution(mesh):
    return jax.shard_map(
        step,
        mesh=mesh,
        in_specs=(
            P("grp", "tok", None),
            P("grp", "tok", None),
            P("grp", "tok", None),
            P("grp", "tok", None),
            P("grp", None),
            P("grp", None),
            P("grp", None),
            P("grp", None),
        ),
        out_specs=(P("grp", "tok", None), P()),
        check_vma=False,
    )
```
